16 devices in a mesh: dp: 2 (over y, z), sp: 8 (over x, core).
Axes of the slice: x: 4, y: 2, z: 1, core: 2. Of those that a mesh axis runs over, the one named last changes fastest.
The devices are a block of a 4x4x8 slice.
Arguments:
- latent: bfloat16 [32, 64, 64, 4], P('dp', 'sp'), parts along dimension 0
- time_emb: bfloat16 [32, 1280], P('dp'), parts along dimension 0
- w_in: bfloat16 [3, 3, 4, 320], replicated
- b_in: bfloat16 [320], replicated
- gn1_scale: bfloat16 [2, 320], replicated
- gn1_shift: bfloat16 [2, 320], replicated
- conv1_w: bfloat16 [2, 3, 3, 320, 320], replicated
- conv1_b: bfloat16 [2, 320], replicated
- temb_w: bfloat16 [2, 1280, 320], replicated
- temb_b: bfloat16 [2, 320], replicated
- gn2_scale: bfloat16 [2, 320], replicated
- gn2_shift: bfloat16 [2, 320], replicated
- conv2_w: bfloat16 [2, 3, 3, 320, 320], replicated
- conv2_b: bfloat16 [2, 320], replicated
- down_w: bfloat16 [3, 3, 320, 320], replicated
- down_b: bfloat16 [320], replicated
Outputs:
- output 1: bfloat16 [32, 64, 64, 320], P('dp', 'sp'), parts along dimension 0
- output 2: bfloat16 [32, 64, 64, 320], P('dp', 'sp'), parts along dimension 0
- output 3: bfloat16 [32, 64, 64, 320], P('dp', 'sp'), parts along dimension 0
- output 4: bfloat16 [32, 32, 32, 320], P('dp', 'sp'), parts along dimension 0
There are 2 independent parts. The reference program is written for one: setup_inputs(seed, part) draws one part's arguments, and reference() takes and returns one part's arrays. A program takes and returns all parts, laid end to end along the dimension named above; an argument that names none is the same for every part.
All inputs are finite; a program needn't handle non-finite values.
Results may differ from the reference program's by a relative error of at most 0.0134522.
Values are sent between devices in bfloat16 or wider.
A program may use at most 768 MiB of HBM per device.

```python
import jax
import jax.numpy as jnp
from jax import lax

BATCH = 16
HEIGHT = 64
WIDTH = 64
CHANNELS = 320
TEMB_DIM = 1280
LATENT_CH = 4
GROUPS = 32
LAYERS = 2
GN_EPS = 1e-5


def setup_inputs(seed: int = 0, part: int = 0) -> dict:
    part_keys = jax.random.split(jax.random.fold_in(jax.random.key(seed), part), 4)
    shared_keys = jax.random.split(jax.random.key(seed + 1), 14)
    row_pos = jnp.linspace(-1.0, 1.0, HEIGHT)[None, :, None, None]
    noise_part = jax.random.normal(part_keys[0], (BATCH, HEIGHT, WIDTH, LATENT_CH), jnp.float32)
    row_slope = 1.5 * jax.random.normal(part_keys[1], (BATCH, 1, 1, LATENT_CH), jnp.float32)
    row_curve = jax.random.normal(part_keys[2], (BATCH, 1, 1, LATENT_CH), jnp.float32)
    latent = noise_part + row_slope * row_pos + row_curve * (1.5 * row_pos * row_pos - 0.5)
    time_emb = jax.random.normal(part_keys[3], (BATCH, TEMB_DIM), jnp.float32)
    conv_std = 1.2 * (9 * CHANNELS) ** -0.5

    def draw_w(key_slot, arr_shape, spread, center):
        return (center + spread * jax.random.normal(shared_keys[key_slot], arr_shape, jnp.float32)).astype(jnp.bfloat16)

    return {
        "latent": latent.astype(jnp.bfloat16),
        "time_emb": time_emb.astype(jnp.bfloat16),
        "w_in": draw_w(0, (3, 3, LATENT_CH, CHANNELS), (9 * LATENT_CH) ** -0.5, 0.0),
        "b_in": draw_w(1, (CHANNELS,), 0.5, 0.0),
        "gn1_scale": draw_w(2, (LAYERS, CHANNELS), 0.3, 1.0),
        "gn1_shift": draw_w(3, (LAYERS, CHANNELS), 0.3, 0.0),
        "conv1_w": draw_w(4, (LAYERS, 3, 3, CHANNELS, CHANNELS), conv_std, 0.0),
        "conv1_b": draw_w(5, (LAYERS, CHANNELS), 0.3, 0.0),
        "temb_w": draw_w(6, (LAYERS, TEMB_DIM, CHANNELS), TEMB_DIM ** -0.5, 0.0),
        "temb_b": draw_w(7, (LAYERS, CHANNELS), 0.3, 0.0),
        "gn2_scale": draw_w(8, (LAYERS, CHANNELS), 0.3, 1.0),
        "gn2_shift": draw_w(9, (LAYERS, CHANNELS), 0.3, 0.0),
        "conv2_w": draw_w(10, (LAYERS, 3, 3, CHANNELS, CHANNELS), conv_std, 0.0),
        "conv2_b": draw_w(11, (LAYERS, CHANNELS), 0.3, 0.0),
        "down_w": draw_w(12, (3, 3, CHANNELS, CHANNELS), (9 * CHANNELS) ** -0.5, 0.0),
        "down_b": draw_w(13, (CHANNELS,), 0.3, 0.0),
    }


def conv_same(inputs, kernel, bias_c, stride):
    out_f32 = lax.conv_general_dilated(inputs[None].astype(jnp.float32), kernel.astype(jnp.float32), (stride, stride), ((1, 1), (1, 1)), dimension_numbers=("NHWC", "HWIO", "NHWC"))
    return (out_f32[0] + bias_c.astype(jnp.float32)).astype(jnp.bfloat16)


def norm_silu(values, gain_c, shift_c):
    grouped = values.reshape(values.shape[0] * values.shape[1], GROUPS, CHANNELS // GROUPS)
    grp_mean = jnp.mean(grouped, axis=(0, 2), keepdims=True)
    grp_var = jnp.mean(jnp.square(grouped - grp_mean), axis=(0, 2), keepdims=True)
    normed = ((grouped - grp_mean) * lax.rsqrt(grp_var + GN_EPS)).reshape(values.shape)
    normed = normed * gain_c.astype(jnp.float32) + shift_c.astype(jnp.float32)
    return jax.nn.silu(normed).astype(jnp.bfloat16)


def reference(latent, time_emb, w_in, b_in, gn1_scale, gn1_shift, conv1_w, conv1_b, temb_w, temb_b, gn2_scale, gn2_shift, conv2_w, conv2_b, down_w, down_b):
    layer_params = (gn1_scale, gn1_shift, conv1_w, conv1_b, temb_w, temb_b, gn2_scale, gn2_shift, conv2_w, conv2_b)

    def one_sample(sample):
        latent_s, temb_s = sample
        first_out = conv_same(latent_s, w_in, b_in, 1)
        emb_act = jax.nn.silu(temb_s.astype(jnp.float32)).astype(jnp.bfloat16)

        def layer_step(hidden, params):
            norm_g1, norm_b1, conv_w1, conv_b1, proj_w, proj_b, norm_g2, norm_b2, conv_w2, conv_b2 = params
            branch = conv_same(norm_silu(hidden.astype(jnp.float32), norm_g1, norm_b1), conv_w1, conv_b1, 1)
            emb_proj = jnp.dot(emb_act.astype(jnp.float32), proj_w.astype(jnp.float32)) + proj_b.astype(jnp.float32)
            mixed_in = branch.astype(jnp.float32) + emb_proj
            branch = conv_same(norm_silu(mixed_in, norm_g2, norm_b2), conv_w2, conv_b2, 1)
            hidden = (hidden.astype(jnp.float32) + branch.astype(jnp.float32)).astype(jnp.bfloat16)
            return hidden, hidden

        last_out, per_layer = lax.scan(layer_step, first_out, layer_params)
        return first_out, per_layer, conv_same(last_out, down_w, down_b, 2)

    firsts, layers_out, down_outs = lax.map(one_sample, (latent, time_emb))
    return firsts, layers_out[:, 0], layers_out[:, 1], down_outs
```

```python
import functools

import jax
import jax.numpy as jnp
from jax import lax
from jax.experimental import pallas as pl
from jax.experimental.pallas import tpu as pltpu
from jax.sharding import PartitionSpec as P

GN_GROUPS = 32
GN_EPS = 1e-5
MESH = pl.DeviceIdType.MESH
F32 = jnp.float32
BF16 = jnp.bfloat16
LANES = 384
MAIN = 256


def lane_ids():
    return lax.broadcasted_iota(jnp.int32, (8, LANES), 1)


def all_sublane_sum(x):
    x = x + pltpu.roll(x, 4, 0)
    x = x + pltpu.roll(x, 2, 0)
    return x + pltpu.roll(x, 1, 0)


def roll_left(x, k):
    return pltpu.roll(x, LANES - k, 1)


def group_window(x):
    x2 = x + roll_left(x, 1)
    x4 = x2 + roll_left(x2, 2)
    x8 = x4 + roll_left(x4, 4)
    return x8 + roll_left(x2, 8)


def group_spread(x):
    x2 = x + pltpu.roll(x, 1, 1)
    x4 = x2 + pltpu.roll(x2, 2, 1)
    x8 = x4 + pltpu.roll(x4, 4, 1)
    return x8 + pltpu.roll(x2, 8, 1)


def kernel(n_sp, count, patches, time_emb, w_in, b_in, gn1_scale, gn1_shift, conv1_b, temb_b, gn2_scale, gn2_shift, conv2_b, down_b,
           conv1_w, conv2_w, temb_w, down_w,
           out0, out1, out2, outd,
           act0, act1, halo, xs_a, xs_b, raw, wmain, wrem, temb_buf, etab, prow, stat_in, stat_out, acc_s, dstage, dbuf,
           halo_recv, stat_recv, halo_send, stat_send, w_sem, t_sem, o_sem):
    n_batch, n_rows, n_cols, chan = act0.shape
    tail = chan - MAIN
    me = lax.axis_index("sp")
    above = lax.rem(me + n_sp - 1, n_sp)
    below = lax.rem(me + 1, n_sp)
    half = n_rows * n_cols
    layers = conv1_w.shape[0]
    acts = (act0, act1)
    xs = (xs_a, xs_b)

    barrier = pltpu.get_barrier_semaphore()
    for d in range(1, n_sp):
        pl.semaphore_signal(barrier, inc=1, device_id={"sp": lax.rem(me + d, n_sp)}, device_id_type=MESH)
    pl.semaphore_wait(barrier, n_sp - 1)

    def w_copy(q):
        src = down_w if q == 2 * layers else (conv1_w, conv2_w)[q % 2].at[q // 2]
        return pltpu.make_async_copy(src, raw.at[q % 2], w_sem.at[q % 2])

    temb_copy = pltpu.make_async_copy(temb_w, temb_buf, t_sem)
    temb_copy.start()
    w_copy(0).start()

    for ref, q0 in ((gn1_scale, 0), (gn2_scale, 1)):
        for l in range(layers):
            prow[3 * (2 * l + q0), :, 0:chan] = jnp.broadcast_to(ref[l:l + 1, :].astype(F32), (8, chan))
    for ref, q0 in ((gn1_shift, 0), (gn2_shift, 1)):
        for l in range(layers):
            prow[3 * (2 * l + q0) + 1, :, 0:chan] = jnp.broadcast_to(ref[l:l + 1, :].astype(F32), (8, chan))
    for ref, q0 in ((conv1_b, 0), (conv2_b, 1)):
        for l in range(layers):
            prow[3 * (2 * l + q0) + 2, :, 0:chan] = jnp.broadcast_to(ref[l:l + 1, :].astype(F32), (8, chan))
    prow[6 * layers, :, 0:chan] = jnp.broadcast_to(b_in[...].astype(F32), (8, chan))
    prow[6 * layers + 1, :, 0:chan] = jnp.broadcast_to(down_b[...].astype(F32), (8, chan))
    for k in range(6 * layers + 2):
        prow[k, :, chan:LANES] = jnp.zeros((8, LANES - chan), F32)
    acc_s[...] = jnp.zeros(acc_s.shape, F32)
    for x in xs:
        x[:, :, 3 * MAIN + 3 * tail:] = jnp.zeros(x.shape[:2] + (x.shape[2] - 3 * MAIN - 3 * tail,), BF16)

    def send_halo(q, s):
        par = q % 2
        up = pltpu.make_async_remote_copy(acts[par].at[s, 0], halo.at[q, s, 1], halo_send.at[s, 0], halo_recv.at[q, s, 1], device_id={"sp": above}, device_id_type=MESH)
        down = pltpu.make_async_remote_copy(acts[par].at[s, n_rows - 1], halo.at[q, s, 0], halo_send.at[s, 1], halo_recv.at[q, s, 0], device_id={"sp": below}, device_id_type=MESH)
        return up, down

    def send_stats(q, s):
        return [pltpu.make_async_remote_copy(stat_out.at[s], stat_in.at[q, s, me], stat_send.at[s, d - 1], stat_recv.at[q, s], device_id={"sp": lax.rem(me + d, n_sp)}, device_id_type=MESH) for d in range(1, n_sp)]

    def wait_sends(s):
        for cp in send_halo(0, s):
            cp.wait_send()
        for cp in send_stats(0, s):
            cp.wait_send()

    def wait_stats(q, s):
        part = stat_in.at[q, s, pl.ds(0, n_sp - 1)]
        pltpu.make_async_copy(part, part, stat_recv.at[q, s]).wait()

    def wait_halo(q, s):
        for k in range(2):
            pltpu.make_async_copy(halo.at[q, s, k], halo.at[q, s, k], halo_recv.at[q, s, k]).wait()

    def put_stats(q, s, k, sums):
        group_ch = chan // GN_GROUPS
        (sm, qm), (st, qt) = sums
        acc_s[2 * k, :, 0:MAIN] = sm
        acc_s[2 * k, :, MAIN:chan] = st
        acc_s[2 * k + 1, :, 0:MAIN] = qm
        acc_s[2 * k + 1, :, MAIN:chan] = qt
        s8 = all_sublane_sum(acc_s[2 * k])
        q8 = all_sublane_sum(acc_s[2 * k + 1])
        sub = lax.broadcasted_iota(jnp.int32, (8, LANES), 0)
        win = group_window(jnp.where(sub < 4, s8, q8))
        lane = lane_ids()
        win = jnp.where((lax.rem(lane, group_ch) == 0) & (lane < chan), win, 0.0)
        row = win[0:1] + pltpu.roll(win, group_ch // 2, 1)[4:5]
        stat_out[s] = row
        stat_in[q, s, me] = row

    def affine(q, s):
        group_ch = chan // GN_GROUPS
        row = jnp.sum(stat_in[q, s], axis=0)
        tot = jnp.broadcast_to(row, (8, LANES))
        lane = lane_ids()
        sub = lax.broadcasted_iota(jnp.int32, (8, LANES), 0)
        rem = lax.rem(lane, group_ch)
        z = jnp.where(sub < 4, jnp.where(rem == 0, tot, 0.0), roll_left(jnp.where(rem == group_ch // 2, tot, 0.0), group_ch // 2))
        z = group_spread(z) * (1.0 / count)
        mean = jnp.broadcast_to(z[0:1], (8, LANES))
        sq = jnp.broadcast_to(z[4:5], (8, LANES))
        inv = lax.rsqrt(sq - mean * mean + GN_EPS)
        scale = inv * prow[3 * q]
        off = prow[3 * q + 1] - mean * scale
        if q % 2:
            off = off + etab[q // 2, s] * scale
        return 0.5 * scale, 0.5 * off

    def act_fn(x, scale, off):
        r, c = x.shape
        z = (x.reshape(r // 8, 8, c) * scale[None] + off[None]).reshape(r, c)
        return z + z * jnp.tanh(z)

    def norm_stage(q, s, dst):
        scale, off = affine(q, s)
        col_m = lax.broadcasted_iota(jnp.int32, (n_cols, MAIN), 0)
        col_t = lax.broadcasted_iota(jnp.int32, (n_cols, tail), 0)

        def shifts(y, col):
            left = jnp.where(col == 0, 0.0, pltpu.roll(y, 1, 0))
            right = jnp.where(col == n_cols - 1, 0.0, pltpu.roll(y, n_cols - 1, 0))
            return left, right

        for r in range(n_rows + 2):
            if r == 0:
                row = halo.at[q, s, 0]
            elif r == n_rows + 1:
                row = halo.at[q, s, 1]
            else:
                row = acts[q % 2].at[s, r - 1]
            ym = act_fn(row[:, 0:MAIN].astype(F32), scale[:, 0:MAIN], off[:, 0:MAIN])
            yt = act_fn(row[:, MAIN:chan].astype(F32), scale[:, MAIN:chan], off[:, MAIN:chan])
            if r == 0:
                keep = jnp.where(me > 0, 1.0, 0.0)
                ym, yt = ym * keep, yt * keep
            if r == n_rows + 1:
                keep = jnp.where(me < n_sp - 1, 1.0, 0.0)
                ym, yt = ym * keep, yt * keep
            lm, rm = shifts(ym, col_m)
            lt, rt = shifts(yt, col_t)
            dst[r, :, 0:MAIN] = lm.astype(BF16)
            dst[r, :, MAIN:2 * MAIN] = ym.astype(BF16)
            dst[r, :, 2 * MAIN:3 * MAIN] = rm.astype(BF16)
            dst[r, :, 3 * MAIN:3 * MAIN + 2 * tail] = jnp.concatenate([lt, yt], axis=1).astype(BF16)
            dst[r, :, 3 * MAIN + 2 * tail:3 * MAIN + 3 * tail] = rt.astype(BF16)

    def col_sums(x):
        v = x.reshape(x.shape[0] // 8, 8, x.shape[1])
        return v.sum(axis=0), (v * v).sum(axis=0)

    def add_pair(a, b):
        return (b if a is None else (a[0] + b[0], a[1] + b[1]))

    def tile_row(x, rows):
        return jnp.broadcast_to(x[None], (rows // 8, 8, x.shape[1])).reshape(rows, x.shape[1])

    def finish(q, s, k, main, rest):
        bias = prow[6 * layers if q < 0 else 3 * q + 2]
        dst = acts[(q + 1) % 2]
        nxt = q + 1
        sums_m = sums_t = None
        for r in range(n_rows):
            rows = slice(r * n_cols, (r + 1) * n_cols)
            tm = (main(r) + tile_row(bias[:, 0:MAIN], n_cols)).astype(BF16)
            tt = (rest(r) + tile_row(bias[:, MAIN:chan], n_cols)).astype(BF16)
            if q >= 0 and q % 2:
                tm = (dst[s, r, :, 0:MAIN].astype(F32) + tm.astype(F32)).astype(BF16)
                tt = (dst[s, r, :, MAIN:chan].astype(F32) + tt.astype(F32)).astype(BF16)
            dst[s, r, :, 0:MAIN] = tm
            dst[s, r, :, MAIN:chan] = tt
            if nxt < 2 * layers:
                vm, vt = tm.astype(F32), tt.astype(F32)
                if nxt % 2:
                    e = etab[nxt // 2, s]
                    vm = vm + tile_row(e[:, 0:MAIN], n_cols)
                    vt = vt + tile_row(e[:, MAIN:chan], n_cols)
                sums_m = add_pair(sums_m, col_sums(vm))
                sums_t = add_pair(sums_t, col_sums(vt))
        if nxt < 2 * layers:
            put_stats(nxt, s, k, (sums_m, sums_t))

    def conv_stage(q, s, k, src):
        lhs = jnp.concatenate([src[dy:dy + n_rows].reshape(half, 4 * MAIN) for dy in range(3)], axis=1)
        main = jnp.dot(lhs, wmain[...], preferred_element_type=F32)
        rest = jnp.dot(src[...].reshape(half + 2 * n_cols, 4 * MAIN), wrem[...], preferred_element_type=F32)

        def main_row(r):
            return main[r * n_cols:(r + 1) * n_cols]

        def rest_row(r):
            p0 = rest[r * n_cols:(r + 1) * n_cols, 0:tail]
            p1 = rest[(r + 1) * n_cols:(r + 2) * n_cols, tail:2 * tail]
            p2 = rest[(r + 2) * n_cols:(r + 3) * n_cols, 2 * tail:3 * tail]
            return p0 + p1 + p2

        finish(q, s, k, main_row, rest_row)

    def start_sends(q, s):
        for cp in send_halo(q, s):
            cp.start()
        if q < 2 * layers:
            for cp in send_stats(q, s):
                cp.start()

    def load_weights(q):
        w_copy(q).wait()
        if q < 2 * layers:
            w_copy(q + 1).start()
        par = q % 2
        for dy in range(3):
            for dx in range(3):
                wmain[dy * 1024 + dx * MAIN:dy * 1024 + (dx + 1) * MAIN, :] = raw[par, dy, dx, 0:MAIN, 0:MAIN]
                wmain[dy * 1024 + 3 * MAIN + dx * tail:dy * 1024 + 3 * MAIN + (dx + 1) * tail, :] = raw[par, dy, dx, MAIN:chan, 0:MAIN]
            wmain[dy * 1024 + 3 * MAIN + 3 * tail:(dy + 1) * 1024, :] = jnp.zeros((MAIN - 3 * tail, MAIN), BF16)
        for dx in range(3):
            for lo, n, at in ((0, MAIN, dx * MAIN), (MAIN, tail, 3 * MAIN + dx * tail)):
                w01 = jnp.concatenate([raw[par, dy, dx, lo:lo + n, MAIN:chan].astype(F32) for dy in range(2)], axis=1)
                wrem[at:at + n, 0:2 * tail] = w01.astype(BF16)
                w2 = jnp.concatenate([raw[par, 2, dx, lo:lo + n, MAIN:chan].astype(F32), jnp.zeros((n, tail), F32)], axis=1)
                wrem[at:at + n, 2 * tail:] = w2.astype(BF16)
        wrem[3 * MAIN + 3 * tail:, :] = jnp.zeros((MAIN - 3 * tail, MAIN), BF16)

    temb_copy.wait()
    emb = time_emb[...].astype(F32)
    emb = (emb * jax.nn.sigmoid(emb)).astype(BF16)
    for l in range(layers):
        e = jnp.dot(emb, temb_buf[l], preferred_element_type=F32) + temb_b[l:l + 1, :].astype(F32)
        for s in range(n_batch):
            etab[l, s, :, 0:chan] = jnp.broadcast_to(e[s:s + 1], (8, chan))
            etab[l, s, :, chan:LANES] = jnp.zeros((8, LANES - chan), F32)

    @pl.loop(0, n_batch // 2)
    def _(j):
        for k in range(2):
            s = 2 * j + k
            out = jnp.dot(patches[s], w_in[...], preferred_element_type=F32)
            finish(-1, s, k, lambda r: out[r * n_cols:(r + 1) * n_cols, 0:MAIN], lambda r: out[r * n_cols:(r + 1) * n_cols, MAIN:chan])
        for k in range(2):
            start_sends(0, 2 * j + k)

    outs = (out0, out1, out2)

    def out_copy(i):
        return pltpu.make_async_copy(act0, outs[i], o_sem)

    out_copy(0).start()
    wait_stats(0, 0)
    wait_halo(0, 0)
    norm_stage(0, 0, xs_a)

    def pair(q, j, last):
        s0 = 2 * j
        targets = [(q, s0 + 1), (q + 1, 0) if last else (q, s0 + 2)]
        for tq, ts in targets:
            if tq < 2 * layers:
                wait_stats(tq, ts)
                wait_halo(tq, ts)
        for k in range(2):
            wait_sends(s0 + k)
        for k in range(2):
            tq, ts = targets[k]
            if tq < 2 * layers:
                norm_stage(tq, ts, xs[1 - k])
            conv_stage(q, s0 + k, k, xs[k])
        for k in range(2):
            start_sends(q + 1, s0 + k)

    for q in range(2 * layers):
        load_weights(q)
        if q % 2:
            out_copy(q // 2).wait()

        @pl.loop(0, n_batch // 2 - 1)
        def _(j):
            pair(q, j, False)

        pair(q, n_batch // 2 - 1, True)
        if q % 2:
            out_copy(q // 2 + 1).start()

    w_copy(2 * layers).wait()
    par = (2 * layers) % 2
    bias = prow[6 * layers + 1]
    half_cols = n_cols // 2
    out_rows = n_rows // 2

    @pl.loop(0, n_batch // 2)
    def _(j):
        for k in range(2):
            for cp in send_halo(0, 2 * j + k):
                cp.wait_send()
            pltpu.make_async_copy(halo.at[2 * layers, 2 * j + k, 1], halo.at[2 * layers, 2 * j + k, 1], halo_recv.at[2 * layers, 2 * j + k, 1]).wait()
            pltpu.make_async_copy(halo.at[2 * layers, 2 * j + k, 0], halo.at[2 * layers, 2 * j + k, 0], halo_recv.at[2 * layers, 2 * j + k, 0]).wait()
        for k in range(2):
            s = 2 * j + k
            for r in range(n_rows + 1):
                row = halo.at[2 * layers, s, 0] if r == 0 else acts[0].at[s, r - 1]
                x = row[...].astype(F32)
                if r == 0:
                    x = x * jnp.where(me > 0, 1.0, 0.0)
                for c in range(3):
                    width = min(128, chan - 128 * c)
                    dstage[k, r, c, :, 0:width] = x[:, 128 * c:128 * c + width]
            for r in range(n_rows + 1):
                evens, odds = [], []
                for c in range(3):
                    width = min(128, chan - 128 * c)
                    evens.append(dstage[k, r, c, pl.ds(0, half_cols, 2), :][:, 0:width])
                    odds.append(dstage[k, r, c, pl.ds(1, half_cols, 2), :][:, 0:width])
                col = lax.broadcasted_iota(jnp.int32, (half_cols, 1), 0)
                lefts = [jnp.where(col == 0, 0.0, pltpu.roll(o, 1, 0)) for o in odds]
                dst = xs[k]
                hc = slice(0, half_cols)
                for at, parts in ((0, lefts), (MAIN, evens), (2 * MAIN, odds)):
                    dst[r, hc, at:at + 128] = parts[0].astype(BF16)
                    dst[r, hc, at + 128:at + 256] = parts[1].astype(BF16)
                dst[r, hc, 3 * MAIN:3 * MAIN + 2 * tail] = jnp.concatenate([lefts[2], evens[2]], axis=1).astype(BF16)
                dst[r, hc, 3 * MAIN + 2 * tail:3 * MAIN + 3 * tail] = odds[2].astype(BF16)
        parts = []
        for k in range(2):
            rows = []
            for ro in range(out_rows):
                rows.append(jnp.concatenate([xs[k][2 * ro + dy, 0:half_cols, :] for dy in range(3)], axis=1))
            parts.append(jnp.concatenate(rows, axis=0))
        lhs = jnp.concatenate(parts, axis=0)
        acc = None
        for dy in range(3):
            for dx in range(3):
                a = jnp.dot(lhs[:, dy * 1024 + dx * MAIN:dy * 1024 + (dx + 1) * MAIN], raw[par, dy, dx, 0:MAIN, :], preferred_element_type=F32)
                acc = a if acc is None else acc + a
            wt = jnp.concatenate([raw[par, dy, dx, MAIN:chan, :] for dx in range(3)] + [jnp.zeros((MAIN - 3 * tail, chan), BF16)], axis=0)
            acc = acc + jnp.dot(lhs[:, dy * 1024 + 3 * MAIN:(dy + 1) * 1024], wt, preferred_element_type=F32)
        acc = acc.reshape(2 * out_rows * half_cols // 8, 8, chan) + bias[None, :, 0:chan]
        dbuf[pl.ds(2 * j, 2)] = acc.astype(BF16).reshape(2, out_rows, half_cols, chan)

    d_copy = pltpu.make_async_copy(dbuf, outd, t_sem)
    d_copy.start()
    out_copy(layers).wait()
    d_copy.wait()


def solution(mesh):
    n_sp = mesh.shape["sp"]
    to_next = [(i, (i + 1) % n_sp) for i in range(n_sp)]
    to_prev = [((i + 1) % n_sp, i) for i in range(n_sp)]

    def band_program(latent, time_emb, w_in, b_in, gn1_scale, gn1_shift, conv1_w, conv1_b, temb_w, temb_b, gn2_scale, gn2_shift, conv2_w, conv2_b, down_w, down_b):
        n_batch, n_rows, n_cols, lat = latent.shape
        chan = w_in.shape[-1]
        layers = conv1_w.shape[0]
        me = lax.axis_index("sp")
        top = lax.ppermute(latent[:, -1:], "sp", to_next[:-1])
        bot = lax.ppermute(latent[:, :1], "sp", to_prev[:-1])
        band = jnp.concatenate([top, latent, bot], axis=1)
        band = jnp.pad(band, ((0, 0), (0, 0), (1, 1), (0, 0)))
        patches = jnp.concatenate([band[:, dy:dy + n_rows, dx:dx + n_cols] for dy in range(3) for dx in range(3)], axis=-1)
        patches = patches.reshape(n_batch, n_rows * n_cols, 9 * lat)
        count = float(n_rows * n_sp * n_cols * (chan // GN_GROUPS))
        vmem = pl.BlockSpec(memory_space=pltpu.VMEM)
        anym = pl.BlockSpec(memory_space=pl.ANY)
        band_shape = jax.ShapeDtypeStruct((n_batch, n_rows, n_cols, chan), BF16)
        down_shape = jax.ShapeDtypeStruct((n_batch, n_rows // 2, n_cols // 2, chan), BF16)
        nq = 2 * layers
        return pl.pallas_call(
            functools.partial(kernel, n_sp, count),
            out_shape=(band_shape,) * 3 + (down_shape,),
            in_specs=[vmem] * 12 + [anym] * 4,
            out_specs=(anym,) * 4,
            scratch_shapes=[
                pltpu.VMEM((n_batch, n_rows, n_cols, chan), BF16),
                pltpu.VMEM((n_batch, n_rows, n_cols, chan), BF16),
                pltpu.VMEM((nq + 1, n_batch, 2, n_cols, chan), BF16),
                pltpu.VMEM((n_rows + 2, n_cols, 4 * MAIN), BF16),
                pltpu.VMEM((n_rows + 2, n_cols, 4 * MAIN), BF16),
                pltpu.VMEM((2, 3, 3, chan, chan), BF16),
                pltpu.VMEM((12 * MAIN, MAIN), BF16),
                pltpu.VMEM((4 * MAIN, MAIN), BF16),
                pltpu.VMEM(temb_w.shape, BF16),
                pltpu.VMEM((layers, n_batch, 8, LANES), F32),
                pltpu.VMEM((6 * layers + 2, 8, LANES), F32),
                pltpu.VMEM((nq, n_batch, n_sp, 1, LANES), F32),
                pltpu.VMEM((n_batch, 1, LANES), F32),
                pltpu.VMEM((4, 8, LANES), F32),
                pltpu.VMEM((2, n_rows + 1, 3, n_cols, 128), F32),
                pltpu.VMEM((n_batch, n_rows // 2, n_cols // 2, chan), BF16),
                pltpu.SemaphoreType.DMA((nq + 1, n_batch, 2)),
                pltpu.SemaphoreType.DMA((nq, n_batch)),
                pltpu.SemaphoreType.DMA((n_batch, 2)),
                pltpu.SemaphoreType.DMA((n_batch, n_sp - 1)),
                pltpu.SemaphoreType.DMA((2,)),
                pltpu.SemaphoreType.DMA,
                pltpu.SemaphoreType.DMA,
            ],
            compiler_params=pltpu.CompilerParams(collective_id=0, has_side_effects=True, vmem_limit_bytes=60 * 1024 * 1024),
        )(patches, time_emb, w_in.reshape(9 * lat, chan), b_in.reshape(1, chan), gn1_scale, gn1_shift, conv1_b, temb_b, gn2_scale, gn2_shift, conv2_b, down_b.reshape(1, chan),
          conv1_w, conv2_w, temb_w, down_w)

    band_spec = P("dp", "sp", None, None)
    return jax.shard_map(band_program, mesh=mesh, in_specs=(band_spec, P("dp", None)) + (P(),) * 14, out_specs=(band_spec,) * 4, check_vma=False)
```
